32 devices in a mesh: groups: 2 (over x), gx: 16 (over z, y, core).
Axes of the slice: x: 2, y: 2, z: 4, core: 2. Of those that a mesh axis runs over, the one named last changes fastest.
Arguments:
- tokens: bfloat16 [768, 4608], P('groups', 'gx'), parts along dimension 0, may hold values from -6 to 6
- gate_weight: bfloat16 [16, 576, 9216], P('gx'), may hold values from -0.09375 to 0.09375
- up_weight: bfloat16 [16, 576, 9216], P('gx'), may hold values from -0.09375 to 0.09375
- down_weight: bfloat16 [16, 2304, 2304], P('gx'), may hold values from -0.046875 to 0.046875
Outputs:
- mixed: bfloat16 [768, 4608], P('groups', 'gx'), parts along dimension 0
The draws below stay inside these ranges and needn't reach their ends.
There are 2 independent parts, one for each index of `groups`. The reference program is written for one: setup_inputs(seed, part) draws one part's arguments, and reference() takes and returns one part's arrays. A program takes and returns all parts, laid end to end along the dimension named above; an argument that names none is the same for every part. Nothing has to cross between parts.
All inputs are finite; a program needn't handle non-finite values.
Results may differ from the reference program's by a relative error of at most 0.015.
Values may be sent and summed in bfloat16 or wider, within the bound.
A program may use at most 128 MiB of HBM per device.

```python
import jax
import jax.numpy as jnp

D = 4608
FF = 18432
TOK = 384
XS = 8
YS = 2


def level_of(own_key, shape, cuts, smallest, top_value):
    gain = 1.0
    for position, parts in cuts:
        draws = jax.random.uniform(jax.random.fold_in(jax.random.fold_in(own_key, 6), position), (parts,), jnp.float32, smallest / len(cuts), top_value / len(cuts))
        gain = gain * jnp.repeat(jnp.exp(draws), shape[position] // parts).reshape((-1,) + (1,) * (len(shape) - 1 - position))
    return gain


def scatter_about(rng, shape, spread, reach, cuts=(), kind=jnp.bfloat16):
    result = spread * jax.random.normal(rng, shape, jnp.float32)
    if cuts:
        result = result * level_of(rng, shape, cuts, -0.22, 0.18)
    return jnp.clip(result, -reach, reach).astype(kind)


def setup_inputs(seed: int = 0, part: int = 0) -> dict:
    splits = jax.random.split(jax.random.key(seed), 5)
    part_splits = jax.random.split(jax.random.fold_in(splits[4], part), 5)
    tokens = scatter_about(part_splits[0], (TOK, D), 1.0, 6.0, ((1, 16),))
    gate_weight = scatter_about(splits[1], (XS * YS, D // XS, FF // YS), D ** -0.5, 0.09375, ((0, 16),))
    up_weight = scatter_about(splits[2], (XS * YS, D // XS, FF // YS), D ** -0.5, 0.09375, ((0, 16),))
    down_weight = scatter_about(splits[3], (XS * YS, FF // XS, D // YS), FF ** -0.5, 0.046875, ((0, 16),))
    return {"tokens": tokens, "gate_weight": gate_weight, "up_weight": up_weight, "down_weight": down_weight}


def assemble(tile_stack, row_count, column_count):
    blocks = tile_stack.reshape(YS, XS, YS, -1, tile_stack.shape[2])
    return blocks.transpose(2, 1, 3, 0, 4).reshape(row_count, column_count)


def reference(tokens, gate_weight, up_weight, down_weight):
    gate_full = assemble(gate_weight, D, FF)
    up_full = assemble(up_weight, D, FF)
    down_full = assemble(down_weight, FF, D)
    gate = jnp.dot(tokens, gate_full, preferred_element_type=jnp.float32)
    up_proj = jnp.dot(tokens, up_full, preferred_element_type=jnp.float32)
    hidden = (jax.nn.gelu(gate, approximate=True) * up_proj).astype(jnp.bfloat16)
    mixed = jnp.dot(hidden, down_full, preferred_element_type=jnp.float32)
    return mixed.astype(jnp.bfloat16)
```

```python
import jax
import jax.numpy as jnp
from jax import lax
from jax.experimental import pallas as pl
from jax.experimental.pallas import tpu as pltpu
from jax.sharding import PartitionSpec as P

XS = 8
CHUNKS = 3
Z_PARTS, ALL_PARTS = 1, 4
VMEM_BYTES = 67043328
MESH = pl.DeviceIdType.MESH
DIAG, ZN, YN, OWN = 0, 1, 2, 3


def from_partner(block, axis, bit):
    count = lax.axis_size(axis)
    route = []
    for low in range(count):
        high = low | 1 << bit
        if high != low and high < count:
            route += [(low, high), (high, low)]
    return lax.ppermute(block, axis, route)


def bit_clear(device_index, bit_number):
    return device_index >> bit_number & 1 == 0


def plain_shards(tokens, gate_weight, up_weight, down_weight):
    gate_tile = gate_weight[0]
    up_tile = up_weight[0]
    down_tile = down_weight[0]
    axis_count = lax.axis_size("gx")
    column_groups = axis_count // XS
    low_bits = XS.bit_length() - 1
    high_bits = column_groups.bit_length() - 1
    device_index = lax.axis_index("gx")
    joined = tokens
    for high_step in range(high_bits):
        bit_number = low_bits + high_step
        partner_piece = from_partner(joined, "gx", bit_number)
        joined = jnp.where(
            bit_clear(device_index, bit_number),
            jnp.concatenate([joined, partner_piece], axis=1),
            jnp.concatenate([partner_piece, joined], axis=1),
        )
    gate_part = jnp.dot(joined, gate_tile, preferred_element_type=jnp.float32)
    up_part = jnp.dot(joined, up_tile, preferred_element_type=jnp.float32)
    stacked = jnp.stack([gate_part, up_part])
    for bit_number in range(low_bits - 1, -1, -1):
        half_width = stacked.shape[2] // 2
        lower_half = stacked[:, :, :half_width]
        upper_half = stacked[:, :, half_width:]
        keep_lower = bit_clear(device_index, bit_number)
        outgoing = jnp.where(keep_lower, upper_half, lower_half)
        kept_half = jnp.where(keep_lower, lower_half, upper_half)
        stacked = kept_half + from_partner(outgoing.astype(jnp.bfloat16), "gx", bit_number).astype(
            outgoing.dtype
        )
    hidden = (jax.nn.gelu(stacked[0], approximate=True) * stacked[1]).astype(jnp.bfloat16)
    hidden_joined = hidden
    for high_step in range(high_bits):
        bit_number = low_bits + high_step
        partner_hidden = from_partner(hidden_joined, "gx", bit_number)
        hidden_joined = jnp.where(
            bit_clear(device_index, bit_number),
            jnp.concatenate([hidden_joined, partner_hidden], axis=1),
            jnp.concatenate([partner_hidden, hidden_joined], axis=1),
        )
    partial_value = jnp.dot(hidden_joined, down_tile, preferred_element_type=jnp.float32)
    for bit_number in range(low_bits - 1, -1, -1):
        half_width = partial_value.shape[1] // 2
        lower_half = partial_value[:, :half_width]
        upper_half = partial_value[:, half_width:]
        keep_lower = bit_clear(device_index, bit_number)
        outgoing = jnp.where(keep_lower, upper_half, lower_half)
        kept_half = jnp.where(keep_lower, lower_half, upper_half)
        partial_value = kept_half + from_partner(
            outgoing.astype(jnp.bfloat16), "gx", bit_number
        ).astype(outgoing.dtype)
    return partial_value.astype(jnp.bfloat16)


def tile_of(width):
    for tiles in range(1, width // 128 + 1):
        if width % tiles == 0 and (width // tiles) % 128 == 0 and width // tiles <= 512:
            return width // tiles
    return 128


def gelu(v):
    return 0.5 * v * (1.0 + jnp.tanh(0.7978845608 * (v + 0.044715 * (v * v * v))))


def kernel(
    tok, gate, up, down, out,
    tok_in, joined, wts, wd, sib_out, sib_in, z1_out, y1_out, z2_out, y2_out,
    z1_in, y1_in, z2_in, y2_in, keep_z, keep_y, keep_o, hid, hid_in,
    acc, blocks, keep_d, dsib_out, dsib_in, dout, din,
    tok_s, tok_r, w_sem, wd_sem, sib_s, sib_r, z1_s, z1_r, y1_s, y1_r,
    z2_s, z2_r, y2_s, y2_r, hid_s, hid_r, dsib_s, dsib_r, dout_s, dout_r,
):
    bf16, f32 = jnp.bfloat16, jnp.float32
    me = lax.axis_index("gx")
    c, yb, zb, a = me % 2, (me // 2) % 2, (me // 4) % 2, me // 8
    chunks = hid.shape[0]
    rows = hid.shape[1]
    feat = tok.shape[1]
    width = hid.shape[2]
    h0 = z1_out.shape[3]
    col = tile_of(width)
    ncol = width // col
    to_c = me + 1 - 2 * c
    to_y = me + 2 - 4 * yb
    to_z = me + 4 - 8 * zb
    to_d = me + 2 - 4 * yb + 4 - 8 * zb
    to_a = me + 8 - 16 * a

    def block_of(kind, core):
        zz = 1 - zb if kind in (DIAG, ZN) else zb
        yy = 1 - yb if kind in (DIAG, YN) else yb
        return zz * 4 + yy * 2 + core

    def remote(src, dst, ss, rs, target):
        return pltpu.make_async_remote_copy(
            src_ref=src, dst_ref=dst, send_sem=ss, recv_sem=rs,
            device_id={"gx": target}, device_id_type=MESH,
        )

    def weight_copies(slot):
        block = block_of(slot // 2, 1 - c if slot % 2 == 0 else c)
        cols = pl.ds(pl.multiple_of(block * width, 128), width)
        return [
            pltpu.make_async_copy(w.at[0, :, cols], wts.at[i, slot], w_sem.at[i, slot])
            for i, w in ((0, gate), (1, up))
        ]

    order = [2 * k for k in range(4)] + [2 * k + 1 for k in range(4)]
    for slot in order:
        for copy in weight_copies(slot):
            copy.start()
    down_copy = pltpu.make_async_copy(down.at[0], wd, wd_sem)
    down_copy.start()

    barrier = pltpu.get_barrier_semaphore()
    for target in (to_c, to_y, to_z, to_d, to_a):
        pl.semaphore_signal(barrier, inc=1, device_id={"gx": target}, device_id_type=MESH)
    pl.semaphore_wait(barrier, 5)

    def tok_copy(s):
        r = pl.ds(s * rows, rows)
        return remote(tok.at[r], tok_in.at[r], tok_s.at[s], tok_r.at[s], to_a)

    for s in range(chunks):
        tok_copy(s).start()

    def join(s):
        tok_copy(s).wait_recv()
        r = pl.ds(s * rows, rows)

        @pl.when(a == 0)
        def _():
            joined[r, 0:feat] = tok[r, :]
            joined[r, feat:2 * feat] = tok_in[r, :]

        @pl.when(a == 1)
        def _():
            joined[r, 0:feat] = tok_in[r, :]
            joined[r, feat:2 * feat] = tok[r, :]

    def each_tile(s, slot, body):
        if s == 0:
            for copy in weight_copies(slot):
                copy.wait()
        lhs = joined.at[pl.ds(s * rows, rows), :]

        def step(t, carry):
            g = t // ncol
            cols = pl.ds(pl.multiple_of((t % ncol) * col, 128), col)
            part = jnp.dot(lhs[...], wts[g, slot, :, cols], preferred_element_type=f32)
            body(g, cols, part)
            return carry

        lax.fori_loop(0, 2 * ncol, step, 0)

    def sib_copy(s, kind):
        return remote(sib_out.at[kind], sib_in.at[s, kind], sib_s.at[s, kind], sib_r.at[s, kind], to_c)

    def sibling(s, kind):
        if s > 0:
            sib_copy(s - 1, kind).wait_send()

        def body(g, cols, part):
            sib_out[kind, g, :, cols] = part.astype(bf16)

        each_tile(s, 2 * kind, body)
        sib_copy(s, kind).start()

    def z1_copy(s, piece):
        return remote(z1_out.at[s % 2, piece], z1_in.at[s, piece], z1_s.at[s, piece], z1_r.at[s, piece], to_z)

    def y1_copy(s, piece):
        return remote(y1_out.at[s % 2, piece], y1_in.at[s, piece], y1_s.at[s, piece], y1_r.at[s, piece], to_y)

    def z2_copy(s):
        return remote(z2_out.at[s % 2], z2_in.at[s], z2_s.at[s], z2_r.at[s], to_z)

    def y2_copy(s):
        return remote(y2_out.at[s % 2], y2_in.at[s], y2_s.at[s], y2_r.at[s], to_y)

    def own(s, kind):
        k = s % 2
        if s >= 2 and kind in (DIAG, ZN):
            z1_copy(s - 2, kind).wait_send()
        if s >= 2 and kind in (DIAG, YN):
            y1_copy(s - 2, 0 if kind == DIAG else 1).wait_send()
        sib_copy(s, kind).wait_recv()

        def body(g, cols, part):
            total = part + sib_in[s, kind, g, :, cols].astype(f32)
            if kind == DIAG:
                z1_out[k, 0, g, :, cols] = total[:h0].astype(bf16)
                y1_out[k, 0, g, :, cols] = total[h0:].astype(bf16)
            elif kind == ZN:
                z1_out[k, 1, g, :, cols] = total[:h0].astype(bf16)
                keep_z[k, g, :, cols] = total[h0:]
            elif kind == YN:
                y1_out[k, 1, g, :, cols] = total[h0:].astype(bf16)
                keep_y[k, g, :, cols] = total[:h0]
            else:
                keep_o[g, :, cols] = total

        each_tile(s, 2 * kind + 1, body)
        if kind == DIAG:
            z1_copy(s, 0).start()
            y1_copy(s, 0).start()
        elif kind == ZN:
            z1_copy(s, 1).start()
        elif kind == YN:
            y1_copy(s, 1).start()

    def loop_cols(body):
        def step(t, carry):
            body(t // ncol, pl.ds(pl.multiple_of((t % ncol) * col, 128), col))
            return carry

        lax.fori_loop(0, 2 * ncol, step, 0)

    def relay(s):
        k = s % 2
        if s >= 2:
            y2_copy(s - 2).wait_send()
            z2_copy(s - 2).wait_send()
        z1_copy(s, 0).wait_recv()

        def to_y2(g, cols):
            y2_out[k, g, :, cols] = (keep_y[k, g, :, cols] + z1_in[s, 0, g, :, cols].astype(f32)).astype(bf16)

        loop_cols(to_y2)
        y2_copy(s).start()
        y1_copy(s, 0).wait_recv()

        def to_z2(g, cols):
            z2_out[k, g, :, cols] = (keep_z[k, g, :, cols] + y1_in[s, 0, g, :, cols].astype(f32)).astype(bf16)

        loop_cols(to_z2)
        z2_copy(s).start()

    def hid_copy(s):
        return remote(hid.at[s], hid_in.at[s], hid_s.at[s], hid_r.at[s], to_a)

    def finish(s):
        own(s, OWN)
        z1_copy(s, 1).wait_recv()
        y1_copy(s, 1).wait_recv()
        y2_copy(s).wait_recv()
        z2_copy(s).wait_recv()

        def step(t, carry):
            cols = pl.ds(pl.multiple_of(t * col, 128), col)
            for r, first, second in (
                (slice(0, h0), z1_in.at[s, 1], y2_in.at[s]),
                (slice(h0, rows), y1_in.at[s, 1], z2_in.at[s]),
            ):
                g, u = (
                    keep_o[i, r, cols] + first[i, :, cols].astype(f32) + second[i, :, cols].astype(f32)
                    for i in (0, 1)
                )
                hid[s, r, cols] = (gelu(g) * u).astype(bf16)
            return carry

        lax.fori_loop(0, ncol, step, 0)
        hid_copy(s).start()

    full = acc.shape[1]
    dcol = tile_of(full)
    dwidth = blocks.shape[2]

    def dsib_copy(s, kind):
        return remote(dsib_out.at[s, kind], dsib_in.at[s, kind], dsib_s.at[s, kind], dsib_r.at[s, kind], to_c)

    def dout_copy(s, kind):
        target = (to_d, to_z, to_y)[kind]
        return remote(dout.at[s, kind], din.at[s, kind], dout_s.at[s, kind], dout_r.at[s, kind], target)

    def project(s):
        if s == 0:
            down_copy.wait()
        first = pl.ds(pl.multiple_of(a * width, 128), width)
        second = pl.ds(pl.multiple_of((1 - a) * width, 128), width)

        def own_half(t, carry):
            cols = pl.ds(pl.multiple_of(t * dcol, 128), dcol)
            acc[:, cols] = jnp.dot(hid[s], wd[first, cols], preferred_element_type=f32)
            return carry

        lax.fori_loop(0, full // dcol, own_half, 0)
        hid_copy(s).wait_recv()

        def other_half(t, carry):
            cols = pl.ds(pl.multiple_of(t * dcol, 128), dcol)
            acc[:, cols] += jnp.dot(hid_in[s], wd[second, cols], preferred_element_type=f32)
            return carry

        lax.fori_loop(0, full // dcol, other_half, 0)
        for b in range(XS):
            blocks[b] = acc[:, b * dwidth:(b + 1) * dwidth]
        for kind in range(4):
            dsib_out[s, kind] = blocks[block_of(kind, 1 - c)].astype(bf16)
            dsib_copy(s, kind).start()

    def spread(s):
        for kind in range(4):
            dsib_copy(s, kind).wait_recv()
            total = blocks[block_of(kind, c)] + dsib_in[s, kind].astype(f32)
            if kind == OWN:
                keep_d[s] = total
            else:
                dout[s, kind] = total.astype(bf16)
                dout_copy(s, kind).start()

    join(0)
    for kind in range(4):
        sibling(0, kind)
    for s in range(chunks):
        if s + 1 < chunks:
            join(s + 1)
        for kind in range(3):
            own(s, kind)
            if s + 1 < chunks:
                sibling(s + 1, kind)
        if s + 1 < chunks:
            sibling(s + 1, OWN)
        if s > 0:
            relay(s - 1)
    if chunks > 1:
        finish(0)
    relay(chunks - 1)
    if chunks == 1:
        finish(0)
    for s in range(chunks):
        project(s)
        if s + 1 < chunks:
            finish(s + 1)
        spread(s)
    for s in range(chunks):
        total = keep_d[s]
        for kind in range(3):
            dout_copy(s, kind).wait_recv()
            total = total + din[s, kind].astype(f32)
        out[pl.ds(s * rows, rows), :] = total.astype(bf16)

    for s in range(chunks):
        tok_copy(s).wait_send()
        hid_copy(s).wait_send()
        for kind in range(4):
            if s == chunks - 1:
                sib_copy(s, kind).wait_send()
            dsib_copy(s, kind).wait_send()
        for kind in range(3):
            dout_copy(s, kind).wait_send()
        if s >= chunks - 2:
            for piece in range(2):
                z1_copy(s, piece).wait_send()
                y1_copy(s, piece).wait_send()
            z2_copy(s).wait_send()
            y2_copy(s).wait_send()


def fused(chunks, tokens, gate_weight, up_weight, down_weight):
    count, feat = tokens.shape
    depth, half = gate_weight.shape[1:]
    deep, full = down_weight.shape[1:]
    rows, width, dwidth = count // chunks, half // XS, full // XS
    h0 = rows // 16 * Z_PARTS // ALL_PARTS * 16
    h1 = rows - h0
    bf16, f32 = jnp.bfloat16, jnp.float32
    v = pltpu.VMEM
    pair = min(chunks, 2)
    buffers = [
        v((count, feat), bf16),
        v((count, 2 * feat), bf16),
        v((2, XS, depth, width), bf16),
        v((deep, full), bf16),
        v((4, 2, rows, width), bf16),
        v((chunks, 4, 2, rows, width), bf16),
        v((pair, 2, 2, h0, width), bf16),
        v((pair, 2, 2, h1, width), bf16),
        v((pair, 2, h1, width), bf16),
        v((pair, 2, h0, width), bf16),
        v((chunks, 2, 2, h0, width), bf16),
        v((chunks, 2, 2, h1, width), bf16),
        v((chunks, 2, h1, width), bf16),
        v((chunks, 2, h0, width), bf16),
        v((pair, 2, h1, width), f32),
        v((pair, 2, h0, width), f32),
        v((2, rows, width), f32),
        v((chunks, rows, width), bf16),
        v((chunks, rows, width), bf16),
        v((rows, full), f32),
        v((XS, rows, dwidth), f32),
        v((chunks, rows, dwidth), f32),
        v((chunks, 4, rows, dwidth), bf16),
        v((chunks, 4, rows, dwidth), bf16),
        v((chunks, 3, rows, dwidth), bf16),
        v((chunks, 3, rows, dwidth), bf16),
    ]
    sem = pltpu.SemaphoreType.DMA
    s = chunks
    shapes = [(s,), (s,), (2, XS), None, (s, 4), (s, 4), (s, 2), (s, 2), (s, 2), (s, 2)]
    shapes += [(s,)] * 6 + [(s, 4), (s, 4), (s, 3), (s, 3)]
    sems = [sem if shape is None else sem(shape) for shape in shapes]
    vmem = pl.BlockSpec(memory_space=pltpu.VMEM)
    hbm = pl.BlockSpec(memory_space=pl.ANY)
    return pl.pallas_call(
        kernel,
        out_shape=jax.ShapeDtypeStruct((count, dwidth), bf16),
        in_specs=[vmem, hbm, hbm, hbm],
        out_specs=vmem,
        scratch_shapes=buffers + sems,
        compiler_params=pltpu.CompilerParams(
            collective_id=0, has_side_effects=True, vmem_limit_bytes=VMEM_BYTES
        ),
    )(tokens, gate_weight, up_weight, down_weight)


def shards(tokens, gate_weight, up_weight, down_weight):
    width = gate_weight.shape[2] // XS
    suits = (
        lax.axis_size("gx") == 2 * XS
        and width % 128 == 0
        and down_weight.shape[2] % 128 == 0
        and tokens.shape[0] % (CHUNKS * 64) == 0
        and tokens.shape[1] % 16 == 0
    )
    if suits:
        return fused(CHUNKS, tokens, gate_weight, up_weight, down_weight)
    return plain_shards(tokens, gate_weight, up_weight, down_weight)


def solution(mesh):
    placed = (P("groups", "gx"), P("gx", None, None), P("gx", None, None), P("gx", None, None))
    return jax.shard_map(
        shards, mesh=mesh, in_specs=placed, out_specs=P("groups", "gx"), check_vma=False
    )
```

```python
import jax
import jax.numpy as jnp
from jax import lax
from jax.experimental import pallas as pl
from jax.experimental.pallas import tpu as pltpu
from jax.sharding import PartitionSpec as P

XS = 8
CHUNKS = 3
Z_PARTS, ALL_PARTS = 3, 8
VMEM_BYTES = 67043328
MESH = pl.DeviceIdType.MESH
DIAG, ZN, YN, OWN = 0, 1, 2, 3


def from_partner(block, axis, bit):
    count = lax.axis_size(axis)
    route = []
    for low in range(count):
        high = low | 1 << bit
        if high != low and high < count:
            route += [(low, high), (high, low)]
    return lax.ppermute(block, axis, route)


def bit_clear(device_index, bit_number):
    return device_index >> bit_number & 1 == 0


def plain_shards(tokens, gate_weight, up_weight, down_weight):
    gate_tile = gate_weight[0]
    up_tile = up_weight[0]
    down_tile = down_weight[0]
    axis_count = lax.axis_size("gx")
    column_groups = axis_count // XS
    low_bits = XS.bit_length() - 1
    high_bits = column_groups.bit_length() - 1
    device_index = lax.axis_index("gx")
    joined = tokens
    for high_step in range(high_bits):
        bit_number = low_bits + high_step
        partner_piece = from_partner(joined, "gx", bit_number)
        joined = jnp.where(
            bit_clear(device_index, bit_number),
            jnp.concatenate([joined, partner_piece], axis=1),
            jnp.concatenate([partner_piece, joined], axis=1),
        )
    gate_part = jnp.dot(joined, gate_tile, preferred_element_type=jnp.float32)
    up_part = jnp.dot(joined, up_tile, preferred_element_type=jnp.float32)
    stacked = jnp.stack([gate_part, up_part])
    for bit_number in range(low_bits - 1, -1, -1):
        half_width = stacked.shape[2] // 2
        lower_half = stacked[:, :, :half_width]
        upper_half = stacked[:, :, half_width:]
        keep_lower = bit_clear(device_index, bit_number)
        outgoing = jnp.where(keep_lower, upper_half, lower_half)
        kept_half = jnp.where(keep_lower, lower_half, upper_half)
        stacked = kept_half + from_partner(outgoing.astype(jnp.bfloat16), "gx", bit_number).astype(
            outgoing.dtype
        )
    hidden = (jax.nn.gelu(stacked[0], approximate=True) * stacked[1]).astype(jnp.bfloat16)
    hidden_joined = hidden
    for high_step in range(high_bits):
        bit_number = low_bits + high_step
        partner_hidden = from_partner(hidden_joined, "gx", bit_number)
        hidden_joined = jnp.where(
            bit_clear(device_index, bit_number),
            jnp.concatenate([hidden_joined, partner_hidden], axis=1),
            jnp.concatenate([partner_hidden, hidden_joined], axis=1),
        )
    partial_value = jnp.dot(hidden_joined, down_tile, preferred_element_type=jnp.float32)
    for bit_number in range(low_bits - 1, -1, -1):
        half_width = partial_value.shape[1] // 2
        lower_half = partial_value[:, :half_width]
        upper_half = partial_value[:, half_width:]
        keep_lower = bit_clear(device_index, bit_number)
        outgoing = jnp.where(keep_lower, upper_half, lower_half)
        kept_half = jnp.where(keep_lower, lower_half, upper_half)
        partial_value = kept_half + from_partner(
            outgoing.astype(jnp.bfloat16), "gx", bit_number
        ).astype(outgoing.dtype)
    return partial_value.astype(jnp.bfloat16)


def tile_of(width):
    for tiles in range(1, width // 128 + 1):
        if width % tiles == 0 and (width // tiles) % 128 == 0 and width // tiles <= 2304:
            return width // tiles
    return 128


def gelu(v):
    return 0.5 * v * (1.0 + jnp.tanh(0.7978845608 * (v + 0.044715 * (v * v * v))))


def kernel(
    tok, gate, up, down, out,
    tok_in, joined, wts, wd, sib_out, sib_in, z1_out, y1_out, z2_out, y2_out,
    z1_in, y1_in, z2_in, y2_in, keep_z, keep_y, keep_o, hid, hid_in,
    acc, blocks, keep_d, dsib_out, dsib_in, dout, din,
    tok_s, tok_r, w_sem, wd_sem, sib_s, sib_r, z1_s, z1_r, y1_s, y1_r,
    z2_s, z2_r, y2_s, y2_r, hid_s, hid_r, dsib_s, dsib_r, dout_s, dout_r,
):
    bf16, f32 = jnp.bfloat16, jnp.float32
    me = lax.axis_index("gx")
    c, yb, zb, a = me % 2, (me // 2) % 2, (me // 4) % 2, me // 8
    chunks = hid.shape[0]
    rows = hid.shape[1]
    feat = tok.shape[1]
    width = hid.shape[2]
    h0 = z1_out.shape[3]
    col = tile_of(width)
    ncol = width // col
    to_c = me + 1 - 2 * c
    to_y = me + 2 - 4 * yb
    to_z = me + 4 - 8 * zb
    to_d = me + 2 - 4 * yb + 4 - 8 * zb
    to_a = me + 8 - 16 * a

    def block_of(kind, core):
        zz = 1 - zb if kind in (DIAG, ZN) else zb
        yy = 1 - yb if kind in (DIAG, YN) else yb
        return zz * 4 + yy * 2 + core

    def remote(src, dst, ss, rs, target):
        return pltpu.make_async_remote_copy(
            src_ref=src, dst_ref=dst, send_sem=ss, recv_sem=rs,
            device_id={"gx": target}, device_id_type=MESH,
        )

    def weight_copies(slot):
        block = block_of(slot // 2, 1 - c if slot % 2 == 0 else c)
        cols = pl.ds(pl.multiple_of(block * width, 128), width)
        return [
            pltpu.make_async_copy(w.at[0, :, cols], wts.at[i, slot], w_sem.at[i, slot])
            for i, w in ((0, gate), (1, up))
        ]

    order = [2 * k for k in range(4)] + [2 * k + 1 for k in range(4)]
    for slot in order:
        for copy in weight_copies(slot):
            copy.start()
    down_copy = pltpu.make_async_copy(down.at[0], wd, wd_sem)
    down_copy.start()

    barrier = pltpu.get_barrier_semaphore()
    for target in (to_c, to_y, to_z, to_d, to_a):
        pl.semaphore_signal(barrier, inc=1, device_id={"gx": target}, device_id_type=MESH)
    pl.semaphore_wait(barrier, 5)

    def tok_copy(s):
        r = pl.ds(s * rows, rows)
        return remote(tok.at[r], tok_in.at[r], tok_s.at[s], tok_r.at[s], to_a)

    for s in range(chunks):
        tok_copy(s).start()

    def join(s):
        tok_copy(s).wait_recv()
        r = pl.ds(s * rows, rows)

        @pl.when(a == 0)
        def _():
            joined[r, 0:feat] = tok[r, :]
            joined[r, feat:2 * feat] = tok_in[r, :]

        @pl.when(a == 1)
        def _():
            joined[r, 0:feat] = tok_in[r, :]
            joined[r, feat:2 * feat] = tok[r, :]

    def each_tile(s, slot, body):
        if s == 0:
            for copy in weight_copies(slot):
                copy.wait()
        lhs = joined.at[pl.ds(s * rows, rows), :]

        def step(t, carry):
            g = t // ncol
            cols = pl.ds(pl.multiple_of((t % ncol) * col, 128), col)
            part = jnp.dot(lhs[...], wts[g, slot, :, cols], preferred_element_type=f32)
            body(g, cols, part)
            return carry

        lax.fori_loop(0, 2 * ncol, step, 0)

    def sib_copy(s, kind):
        return remote(sib_out.at[kind], sib_in.at[s, kind], sib_s.at[s, kind], sib_r.at[s, kind], to_c)

    def sibling(s, kind):
        if s > 0:
            sib_copy(s - 1, kind).wait_send()

        def body(g, cols, part):
            sib_out[kind, g, :, cols] = part.astype(bf16)

        each_tile(s, 2 * kind, body)
        sib_copy(s, kind).start()

    def z1_copy(s, piece):
        return remote(z1_out.at[s % 2, piece], z1_in.at[s, piece], z1_s.at[s, piece], z1_r.at[s, piece], to_z)

    def y1_copy(s, piece):
        return remote(y1_out.at[s % 2, piece], y1_in.at[s, piece], y1_s.at[s, piece], y1_r.at[s, piece], to_y)

    def z2_copy(s):
        return remote(z2_out.at[s % 2], z2_in.at[s], z2_s.at[s], z2_r.at[s], to_z)

    def y2_copy(s):
        return remote(y2_out.at[s % 2], y2_in.at[s], y2_s.at[s], y2_r.at[s], to_y)

    def own(s, kind):
        k = s % 2
        if s >= 2 and kind in (DIAG, ZN):
            z1_copy(s - 2, kind).wait_send()
        if s >= 2 and kind in (DIAG, YN):
            y1_copy(s - 2, 0 if kind == DIAG else 1).wait_send()
        sib_copy(s, kind).wait_recv()

        def body(g, cols, part):
            total = part + sib_in[s, kind, g, :, cols].astype(f32)
            if kind == DIAG:
                z1_out[k, 0, g, :, cols] = total[:h0].astype(bf16)
                y1_out[k, 0, g, :, cols] = total[h0:].astype(bf16)
            elif kind == ZN:
                z1_out[k, 1, g, :, cols] = total[:h0].astype(bf16)
                keep_z[k, g, :, cols] = total[h0:]
            elif kind == YN:
                y1_out[k, 1, g, :, cols] = total[h0:].astype(bf16)
                keep_y[k, g, :, cols] = total[:h0]
            else:
                keep_o[g, :, cols] = total

        each_tile(s, 2 * kind + 1, body)
        if kind == DIAG:
            z1_copy(s, 0).start()
            y1_copy(s, 0).start()
        elif kind == ZN:
            z1_copy(s, 1).start()
        elif kind == YN:
            y1_copy(s, 1).start()

    def loop_cols(body):
        def step(t, carry):
            body(t // ncol, pl.ds(pl.multiple_of((t % ncol) * col, 128), col))
            return carry

        lax.fori_loop(0, 2 * ncol, step, 0)

    def relay(s):
        k = s % 2
        if s >= 2:
            y2_copy(s - 2).wait_send()
            z2_copy(s - 2).wait_send()
        z1_copy(s, 0).wait_recv()

        def to_y2(g, cols):
            y2_out[k, g, :, cols] = (keep_y[k, g, :, cols] + z1_in[s, 0, g, :, cols].astype(f32)).astype(bf16)

        loop_cols(to_y2)
        y2_copy(s).start()
        y1_copy(s, 0).wait_recv()

        def to_z2(g, cols):
            z2_out[k, g, :, cols] = (keep_z[k, g, :, cols] + y1_in[s, 0, g, :, cols].astype(f32)).astype(bf16)

        loop_cols(to_z2)
        z2_copy(s).start()

    def hid_copy(s):
        return remote(hid.at[s], hid_in.at[s], hid_s.at[s], hid_r.at[s], to_a)

    def finish(s):
        own(s, OWN)
        z1_copy(s, 1).wait_recv()
        y1_copy(s, 1).wait_recv()
        y2_copy(s).wait_recv()
        z2_copy(s).wait_recv()

        def step(t, carry):
            cols = pl.ds(pl.multiple_of(t * col, 128), col)
            for r, first, second in (
                (slice(0, h0), z1_in.at[s, 1], y2_in.at[s]),
                (slice(h0, rows), y1_in.at[s, 1], z2_in.at[s]),
            ):
                g, u = (
                    keep_o[i, r, cols] + first[i, :, cols].astype(f32) + second[i, :, cols].astype(f32)
                    for i in (0, 1)
                )
                hid[s, r, cols] = (gelu(g) * u).astype(bf16)
            return carry

        lax.fori_loop(0, ncol, step, 0)
        hid_copy(s).start()

    full = acc.shape[1]
    dcol = tile_of(full)
    dwidth = blocks.shape[2]

    def dsib_copy(s, kind):
        return remote(dsib_out.at[s, kind], dsib_in.at[s, kind], dsib_s.at[s, kind], dsib_r.at[s, kind], to_c)

    def dout_copy(s, kind):
        target = (to_d, to_z, to_y)[kind]
        return remote(dout.at[s, kind], din.at[s, kind], dout_s.at[s, kind], dout_r.at[s, kind], target)

    def project(s):
        if s == 0:
            down_copy.wait()
        first = pl.ds(pl.multiple_of(a * width, 128), width)
        second = pl.ds(pl.multiple_of((1 - a) * width, 128), width)

        def own_half(t, carry):
            cols = pl.ds(pl.multiple_of(t * dcol, 128), dcol)
            acc[:, cols] = jnp.dot(hid[s], wd[first, cols], preferred_element_type=f32)
            return carry

        lax.fori_loop(0, full // dcol, own_half, 0)
        hid_copy(s).wait_recv()

        def other_half(t, carry):
            cols = pl.ds(pl.multiple_of(t * dcol, 128), dcol)
            acc[:, cols] += jnp.dot(hid_in[s], wd[second, cols], preferred_element_type=f32)
            return carry

        lax.fori_loop(0, full // dcol, other_half, 0)
        for b in range(XS):
            blocks[b] = acc[:, b * dwidth:(b + 1) * dwidth]
        for kind in range(4):
            dsib_out[s, kind] = blocks[block_of(kind, 1 - c)].astype(bf16)
            dsib_copy(s, kind).start()

    def spread(s):
        for kind in range(4):
            dsib_copy(s, kind).wait_recv()
            total = blocks[block_of(kind, c)] + dsib_in[s, kind].astype(f32)
            if kind == OWN:
                keep_d[s] = total
            else:
                dout[s, kind] = total.astype(bf16)
                dout_copy(s, kind).start()

    join(0)
    for kind in range(4):
        sibling(0, kind)
    for s in range(chunks):
        for kind in range(3):
            own(s, kind)
        if s + 1 < chunks:
            join(s + 1)
            for kind in range(4):
                sibling(s + 1, kind)
        if s > 0:
            finish(s - 1)
        relay(s)
    for s in range(chunks):
        if s < chunks - 1:
            project(s)
        if s == max(chunks - 2, 0):
            finish(chunks - 1)
        if s == chunks - 1:
            project(s)
        spread(s)
    for s in range(chunks):
        total = keep_d[s]
        for kind in range(3):
            dout_copy(s, kind).wait_recv()
            total = total + din[s, kind].astype(f32)
        out[pl.ds(s * rows, rows), :] = total.astype(bf16)

    for s in range(chunks):
        tok_copy(s).wait_send()
        hid_copy(s).wait_send()
        for kind in range(4):
            if s == chunks - 1:
                sib_copy(s, kind).wait_send()
            dsib_copy(s, kind).wait_send()
        for kind in range(3):
            dout_copy(s, kind).wait_send()
        if s >= chunks - 2:
            for piece in range(2):
                z1_copy(s, piece).wait_send()
                y1_copy(s, piece).wait_send()
            z2_copy(s).wait_send()
            y2_copy(s).wait_send()


def fused(chunks, tokens, gate_weight, up_weight, down_weight):
    count, feat = tokens.shape
    depth, half = gate_weight.shape[1:]
    deep, full = down_weight.shape[1:]
    rows, width, dwidth = count // chunks, half // XS, full // XS
    h0 = rows // 16 * Z_PARTS // ALL_PARTS * 16
    h1 = rows - h0
    bf16, f32 = jnp.bfloat16, jnp.float32
    v = pltpu.VMEM
    pair = min(chunks, 2)
    buffers = [
        v((count, feat), bf16),
        v((count, 2 * feat), bf16),
        v((2, XS, depth, width), bf16),
        v((deep, full), bf16),
        v((4, 2, rows, width), bf16),
        v((chunks, 4, 2, rows, width), bf16),
        v((pair, 2, 2, h0, width), bf16),
        v((pair, 2, 2, h1, width), bf16),
        v((pair, 2, h1, width), bf16),
        v((pair, 2, h0, width), bf16),
        v((chunks, 2, 2, h0, width), bf16),
        v((chunks, 2, 2, h1, width), bf16),
        v((chunks, 2, h1, width), bf16),
        v((chunks, 2, h0, width), bf16),
        v((pair, 2, h1, width), f32),
        v((pair, 2, h0, width), f32),
        v((2, rows, width), f32),
        v((chunks, rows, width), bf16),
        v((chunks, rows, width), bf16),
        v((rows, full), f32),
        v((XS, rows, dwidth), f32),
        v((chunks, rows, dwidth), f32),
        v((chunks, 4, rows, dwidth), bf16),
        v((chunks, 4, rows, dwidth), bf16),
        v((chunks, 3, rows, dwidth), bf16),
        v((chunks, 3, rows, dwidth), bf16),
    ]
    sem = pltpu.SemaphoreType.DMA
    s = chunks
    shapes = [(s,), (s,), (2, XS), None, (s, 4), (s, 4), (s, 2), (s, 2), (s, 2), (s, 2)]
    shapes += [(s,)] * 6 + [(s, 4), (s, 4), (s, 3), (s, 3)]
    sems = [sem if shape is None else sem(shape) for shape in shapes]
    vmem = pl.BlockSpec(memory_space=pltpu.VMEM)
    hbm = pl.BlockSpec(memory_space=pl.ANY)
    return pl.pallas_call(
        kernel,
        out_shape=jax.ShapeDtypeStruct((count, dwidth), bf16),
        in_specs=[vmem, hbm, hbm, hbm],
        out_specs=vmem,
        scratch_shapes=buffers + sems,
        compiler_params=pltpu.CompilerParams(
            collective_id=0, has_side_effects=True, vmem_limit_bytes=VMEM_BYTES
        ),
    )(tokens, gate_weight, up_weight, down_weight)


def shards(tokens, gate_weight, up_weight, down_weight):
    width = gate_weight.shape[2] // XS
    suits = (
        lax.axis_size("gx") == 2 * XS
        and width % 128 == 0
        and down_weight.shape[2] % 128 == 0
        and tokens.shape[0] % (CHUNKS * 64) == 0
        and tokens.shape[1] % 16 == 0
    )
    if suits:
        return fused(CHUNKS, tokens, gate_weight, up_weight, down_weight)
    return plain_shards(tokens, gate_weight, up_weight, down_weight)


def solution(mesh):
    placed = (P("groups", "gx"), P("gx", None, None), P("gx", None, None), P("gx", None, None))
    return jax.shard_map(
        shards, mesh=mesh, in_specs=placed, out_specs=P("groups", "gx"), check_vma=False
    )
```
